32 devices in a mesh: inner: 4 (over y, core), outer: 8 (over z, x).
Axes of the slice: x: 2, y: 2, z: 4, core: 2. Of those that a mesh axis runs over, the one named last changes fastest.
Arguments:
- query_rows: bfloat16 [16384, 512], P(('outer', 'inner')), may hold values from -6 to 6
- key_rows: bfloat16 [16384, 512], P(('outer', 'inner')), may hold values from -6 to 6
- value_rows: bfloat16 [16384, 512], P(('outer', 'inner')), may hold values from -6 to 6
- level_ids: int32 [16384], P(('outer', 'inner')), may hold values from 0 to 15
- level_table: float32 [16, 16, 4], replicated, may hold values from 0.1 to 1
Outputs:
- attended: bfloat16 [16384, 512], P(('outer', 'inner'))
The draws below stay inside these ranges and needn't reach their ends.
All inputs are finite; a program needn't handle non-finite values.
Results may differ from the reference program's by a relative error of at most 0.0049.
Values sent between devices are 32-bit elements; how exact they have to be, the bound alone decides.
No kernel may reach another device: no remote copies, remote signals or barrier semaphores. Data moves between devices by JAX's collectives and lax.ppermute only.
A program may use at most 64 MiB of HBM per device.

```python
import math
import jax
import jax.numpy as jnp
from jax import lax

HEADS = 4
HD = 128
SPAN = 128
LEVELS = 16
CLASSES = 16
TOK_DEV = 512
TOKENS = 16384
N_INNER = 4
N_OUTER = 8


def plant(entries, key, low, top_value):
    longest = entries.shape.index(max(entries.shape))
    spots = []
    for shift in (0, 1):
        where = [jax.random.randint(jax.random.fold_in(key, axis), (), 0, length) for axis, length in enumerate(entries.shape)]
        where[longest] = (where[longest] + shift) % entries.shape[longest]
        spots.append(tuple(where))
    return entries.at[spots[0]].set(low).at[spots[1]].set(top_value)


def block_scale(own_key, extent, split, smallest, top_value):
    def one(axis_at, blocks):
        steps = jax.random.uniform(jax.random.fold_in(jax.random.fold_in(own_key, 6), axis_at), (blocks,), jnp.float32, smallest / len(split), top_value / len(split))
        return jnp.repeat(jnp.exp(steps), extent[axis_at] // blocks).reshape((-1,) + (1,) * (len(extent) - axis_at - 1))

    gain = one(*split[0])
    for cut in split[1:]:
        gain = gain * one(*cut)
    return gain


def gaussian(key, dims, spread, limit, cuts=(), kind=jnp.bfloat16):
    array = jax.random.normal(key, dims, jnp.float32) * spread
    if len(cuts) > 0:
        array = block_scale(key, dims, cuts, -0.22, 0.18) * array
    return jnp.clip(array, min=-limit, max=limit).astype(kind)


def setup_inputs(seed: int = 0) -> dict:
    arg_keys = jax.random.split(jax.random.key(seed), 6)
    return {
        "query_rows": gaussian(arg_keys[0], (TOKENS, HEADS * HD), 1.0, 6.0, ((0, 32),)),
        "key_rows": gaussian(arg_keys[1], (TOKENS, HEADS * HD), 1.0, 6.0, ((0, 32),)),
        "value_rows": gaussian(arg_keys[2], (TOKENS, HEADS * HD), 1.0, 6.0, ((0, 32),)),
        "level_ids": plant(jax.random.randint(arg_keys[3], (TOKENS,), 0, CLASSES), jax.random.fold_in(arg_keys[3], 1), 0, CLASSES - 1).astype(jnp.int32),
        "level_table": jnp.clip(jnp.exp(jax.random.uniform(arg_keys[4], (CLASSES, LEVELS, HEADS), jnp.float32, math.log(0.1), math.log(1.0))), 0.1, 1.0),
    }


norm_eps = 1e-06
precise = lax.Precision.HIGHEST

def left_selectors(count, own_rows, level_bits):
    columns = jnp.arange(count, dtype=jnp.int32)
    result = []
    for bit_pos in range(level_bits):
        lower = own_rows >> bit_pos + 1 << bit_pos + 1
        upper = own_rows >> bit_pos << bit_pos
        active = own_rows >> bit_pos & 1 == 1
        inside = (columns[None, :] >= lower[:, None]) & (columns[None, :] < upper[:, None]) & active[:, None]
        result.append(inside.astype(jnp.float32))
    return result

def local_output(query_rows, key_rows, value_rows, weights_tok, cross_states):
    token_count = query_rows.shape[0]
    span_count = token_count // SPAN
    level_bits = span_count.bit_length() - 1
    shape_four = (span_count, SPAN, HEADS, HD)
    query_blocks = query_rows.reshape(shape_four).astype(jnp.float32)
    key_blocks = key_rows.reshape(shape_four).astype(jnp.float32)
    value_blocks = value_rows.reshape(shape_four).astype(jnp.float32)
    level_blocks = weights_tok.reshape(span_count, SPAN, LEVELS, HEADS)
    span_states = jnp.einsum('cthd,cthe->chde', key_blocks, value_blocks)
    scores = jnp.einsum('cthd,cshd->chts', query_blocks, key_blocks)
    position = jnp.arange(SPAN, dtype=jnp.int32)
    causal = position[:, None] >= position[None, :]
    scale_now = jnp.transpose(level_blocks[:, :, 0, :], (0, 2, 1))[..., None]
    weighted = lax.optimization_barrier(jnp.where(causal, scores * scale_now, 0.0).astype(jnp.bfloat16))
    unnormed = jnp.einsum('chts,cshd->cthd', weighted.astype(jnp.float32), value_blocks)
    flat = span_states.reshape(span_count, -1)
    selectors = left_selectors(span_count, jnp.arange(span_count, dtype=jnp.int32), level_bits)
    for bit_pos in range(level_bits):
        left_block = jnp.dot(selectors[bit_pos], flat, precision=precise).reshape(span_states.shape)
        left_block = lax.optimization_barrier(left_block.astype(jnp.bfloat16)).astype(jnp.float32)
        partial_out = jnp.einsum('cthd,chde->cthe', query_blocks, left_block)
        unnormed = unnormed + level_blocks[:, :, 1 + bit_pos, :, None] * partial_out
    unnormed = unnormed.reshape(token_count, HEADS, HD)
    query_heads = query_rows.reshape(token_count, HEADS, HD).astype(jnp.float32)
    for bit_pos in range(len(cross_states)):
        partial_out = jnp.einsum('thd,hde->the', query_heads, cross_states[bit_pos].astype(jnp.float32))
        unnormed = unnormed + weights_tok[:, 1 + level_bits + bit_pos, :, None] * partial_out
    mean_square = lax.optimization_barrier(jnp.mean(unnormed * unnormed, axis=-1, keepdims=True))
    normed = unnormed * lax.rsqrt(mean_square + norm_eps)
    return normed.reshape(token_count, HEADS * HD).astype(jnp.bfloat16)

def reference(query_rows, key_rows, value_rows, level_ids, level_table):
    shards = N_INNER * N_OUTER
    cross_bits = shards.bit_length() - 1
    shard_ids = jnp.arange(shards, dtype=jnp.int32)

    def shard_state(shard):
        start = (shard * TOK_DEV).astype(jnp.int32)
        keys_here = lax.dynamic_slice_in_dim(key_rows, start, TOK_DEV, 0).reshape(TOK_DEV, HEADS, HD)
        values_here = lax.dynamic_slice_in_dim(value_rows, start, TOK_DEV, 0).reshape(TOK_DEV, HEADS, HD)
        return jnp.einsum('thd,the->hde', keys_here.astype(jnp.float32), values_here.astype(jnp.float32))
    states = lax.map(shard_state, shard_ids)
    prefix = jnp.concatenate([jnp.zeros((1, HEADS, HD, HD), jnp.float32), jnp.cumsum(states, axis=0)], axis=0)

    def shard_out(shard):
        start = (shard * TOK_DEV).astype(jnp.int32)
        queries_here = lax.dynamic_slice_in_dim(query_rows, start, TOK_DEV, 0)
        keys_here = lax.dynamic_slice_in_dim(key_rows, start, TOK_DEV, 0)
        values_here = lax.dynamic_slice_in_dim(value_rows, start, TOK_DEV, 0)
        ids_here = lax.dynamic_slice_in_dim(level_ids, start, TOK_DEV, 0)
        weights_tok = level_table[ids_here]
        cross_states = []
        for bit_pos in range(cross_bits):
            upper = shard >> bit_pos << bit_pos
            lower = shard >> bit_pos + 1 << bit_pos + 1
            active = (shard >> bit_pos & 1).astype(jnp.float32)
            cross_states.append(((prefix[upper] - prefix[lower]) * active).astype(jnp.bfloat16))
        return local_output(queries_here, keys_here, values_here, weights_tok, cross_states)
    blocks = lax.map(shard_out, shard_ids)
    return blocks.reshape(TOKENS, HEADS * HD)
```

```python
import functools

import jax
import jax.numpy as jnp
from jax import lax
from jax.experimental import pallas as pl
from jax.experimental.pallas import tpu as pltpu
from jax.sharding import PartitionSpec as P

HEADS = 4
HD = 128
SPAN = 128
LEVELS = 16
HALF = HEADS // 2

norm_eps = 1e-06


def core_parity():
    return lax.rem(lax.axis_index("inner"), 2)


def half_columns(side, head):
    core = core_parity()
    which = core if side == 0 else 1 - core
    return pl.ds(pl.multiple_of((which * HALF + head) * HD, HD), HD)


def state_of(keys, values):
    return lax.dot_general(keys, values, (((0,), (0,)), ((), ())), preferred_element_type=jnp.float32)


def dot(left, right):
    return lax.dot_general(left, right, (((1,), (0,)), ((), ())), preferred_element_type=jnp.float32)


def states_kernel(key_ref, value_ref, other_ref, own_ref):
    for side, out_ref in ((1, other_ref), (0, own_ref)):
        for head in range(HALF):
            columns = half_columns(side, head)
            out_ref[head] = state_of(key_ref[:, columns], value_ref[:, columns])


def local_kernel(query_ref, key_ref, value_ref, ids_ref, table_ref, acc_ref, weights_ref):
    token_count = query_ref.shape[0]
    span_count = token_count // SPAN
    level_bits = span_count.bit_length() - 1
    classes = table_ref.shape[0]
    onehot = (ids_ref[...] == lax.broadcasted_iota(jnp.int32, (token_count, classes), 1)).astype(jnp.float32)
    weights = lax.dot_general(
        onehot,
        table_ref[...],
        (((1,), (0,)), ((), ())),
        precision=lax.Precision.HIGHEST,
        preferred_element_type=jnp.float32,
    )
    weights_ref[...] = weights
    causal = lax.broadcasted_iota(jnp.int32, (SPAN, SPAN), 0) >= lax.broadcasted_iota(jnp.int32, (SPAN, SPAN), 1)
    for head in range(HEADS):
        columns = slice(head * HD, (head + 1) * HD)
        states = [
            state_of(key_ref[c * SPAN : (c + 1) * SPAN, columns], value_ref[c * SPAN : (c + 1) * SPAN, columns])
            for c in range(span_count - 1)
        ]
        for c in range(span_count):
            rows = slice(c * SPAN, (c + 1) * SPAN)
            query = query_ref[rows, columns]
            scores = lax.dot_general(
                query, key_ref[rows, columns], (((1,), (1,)), ((), ())), preferred_element_type=jnp.float32
            )
            scaled = jnp.where(causal, scores * weights[rows, head : head + 1], 0.0)
            total = dot(scaled.astype(jnp.bfloat16), value_ref[rows, columns])
            for bit in range(level_bits):
                if c >> bit & 1:
                    first = c >> bit + 1 << bit + 1
                    left = functools.reduce(jnp.add, states[first : first + (1 << bit)])
                    at = (1 + bit) * HEADS + head
                    total = total + weights[rows, at : at + 1] * dot(query, left.astype(jnp.bfloat16))
            acc_ref[rows, columns] = total


def shard_active(bit, inner_bits):
    if bit < inner_bits:
        return lax.rem(lax.axis_index("inner") >> bit, 2)
    return lax.rem(lax.axis_index("outer") >> bit - inner_bits, 2)


def level_weight(weights_ref, side, level, head):
    at = level * HEADS + head
    low, high = weights_ref[:, at : at + 1], weights_ref[:, at + HALF : at + HALF + 1]
    return jnp.where(core_parity() == side, low, high)


def add_levels(total, query, weights_ref, side, head, level_bits, inner_bits, lefts):
    for bit, left in lefts:
        active = shard_active(bit, inner_bits).astype(jnp.float32)
        left = (left * active).astype(jnp.bfloat16)
        total = total + level_weight(weights_ref, side, 1 + level_bits + bit, head) * dot(query, left)
    return total


def cross_kernel(side, level_bits, inner_bits, bits, query_ref, weights_ref, acc_ref, *refs):
    lefts, out_ref = refs[:-1], refs[-1]
    for head in range(HALF):
        columns = half_columns(side, head)
        out_ref[:, head * HD : (head + 1) * HD] = add_levels(
            acc_ref[:, columns], query_ref[:, columns], weights_ref, side, head, level_bits, inner_bits,
            [(bit, ref[head]) for bit, ref in zip(bits, lefts)],
        )


def normed(total):
    mean_square = jnp.mean(total * total, axis=-1, keepdims=True)
    return (total * lax.rsqrt(mean_square + norm_eps)).astype(jnp.bfloat16)


def last_own_kernel(level_bits, inner_bits, bit, query_ref, weights_ref, acc_ref, left_ref, out_ref):
    for head in range(HALF):
        columns = half_columns(0, head)
        mine = slice(head * HD, (head + 1) * HD)
        out_ref[:, mine] = normed(add_levels(
            acc_ref[:, mine], query_ref[:, columns], weights_ref, 0, head, level_bits, inner_bits,
            [(bit, left_ref[head])],
        ))


def last_other_kernel(level_bits, inner_bits, bit, query_ref, weights_ref, acc_ref, left_ref, own_ref, out_ref):
    for head in range(HALF):
        mine = slice(head * HD, (head + 1) * HD)
        out_ref[:, half_columns(0, head)] = own_ref[:, mine]
        columns = half_columns(1, head)
        out_ref[:, columns] = normed(add_levels(
            acc_ref[:, mine], query_ref[:, columns], weights_ref, 1, head, level_bits, inner_bits,
            [(bit, left_ref[head])],
        ))


def call(kernel, out_shape, *args, flops=0, name=None):
    whole = pl.BlockSpec(memory_space=pltpu.VMEM)
    many = isinstance(out_shape, (tuple, list))
    moved = sum(a.size * a.dtype.itemsize for a in args)
    return pl.pallas_call(
        kernel,
        out_shape=out_shape,
        in_specs=[whole] * len(args),
        out_specs=tuple([whole] * len(out_shape)) if many else whole,
        compiler_params=pltpu.CompilerParams(vmem_limit_bytes=24 * 1024 * 1024),
        cost_estimate=pl.CostEstimate(flops=flops, bytes_accessed=moved, transcendentals=0),
        name=name,
    )(*args)


def swap(value, axis, mask):
    return lax.ppermute(value, axis, [(i, i ^ mask) for i in range(lax.axis_size(axis))])


def on_device(query_rows, key_rows, value_rows, level_ids, level_table):
    token_count, width = query_rows.shape
    classes = level_table.shape[0]
    level_bits = (token_count // SPAN).bit_length() - 1
    inner_bits = lax.axis_size("inner").bit_length() - 1
    outer_bits = lax.axis_size("outer").bit_length() - 1
    bits = inner_bits + outer_bits
    f32 = functools.partial(jax.ShapeDtypeStruct, dtype=jnp.float32)
    bf16 = functools.partial(jax.ShapeDtypeStruct, dtype=jnp.bfloat16)
    half_state = f32((HALF, HD, HD))

    other, own = call(states_kernel, (half_state, half_state), key_rows, value_rows, name="states")
    received = [swap(other, "inner", 1)]
    total = own + received[0]
    for bit in range(1, bits):
        if bit < inner_bits:
            arrived = swap(total, "inner", 1 << bit)
        else:
            at = bit - inner_bits
            mask = 3 << at - 1 if at == outer_bits - 1 and at > 0 else 1 << at
            arrived = swap(total, "outer", mask)
        received.append(arrived)
        total = total + arrived

    acc, weights = call(
        local_kernel,
        (f32((token_count, width)), f32((token_count, LEVELS * HEADS))),
        query_rows, key_rows, value_rows, level_ids[:, None], level_table.reshape(classes, -1),
        name="local",
    )
    early = list(range(bits - 1))
    half_acc = f32((token_count, HALF * HD))
    acc_own = call(
        functools.partial(cross_kernel, 0, level_bits, inner_bits, early),
        half_acc, query_rows, weights, acc, *received[:-1], name="cross_own",
    )
    gathered = swap(jnp.concatenate([own] + received[1:-1], axis=0), "inner", 1)
    acc_other = call(
        functools.partial(cross_kernel, 1, level_bits, inner_bits, early),
        half_acc, query_rows, weights, acc,
        *[gathered[HALF * i : HALF * (i + 1)] for i in early], name="cross_other",
    )
    last = bits - 1
    last_other = swap(received[-1], "inner", 1)
    out_own = call(
        functools.partial(last_own_kernel, level_bits, inner_bits, last),
        bf16((token_count, HALF * HD)), query_rows, weights, acc_own, received[-1], name="last_own",
    )
    return call(
        functools.partial(last_other_kernel, level_bits, inner_bits, last),
        bf16((token_count, width)), query_rows, weights, acc_other, last_other, out_own, name="last_other",
    )


def solution(mesh):
    rows = P(("outer", "inner"), None)
    return jax.shard_map(
        on_device,
        mesh=mesh,
        in_specs=(rows, rows, rows, P(("outer", "inner")), P()),
        out_specs=rows,
        check_vma=False,
    )
```
